256 devices in a mesh: units: 64 (over x, z, core), expert: 4 (over y).
Axes of the slice: x: 4, y: 4, z: 8, core: 2. Of those that a mesh axis runs over, the one named last changes fastest.
Arguments:
- a_up: float32 [57344, 2048], P(('expert', 'units')), parts along dimension 0, may hold values from -6 to 6
- a_down: float32 [57344, 2048], P(('expert', 'units')), parts along dimension 0, may hold values from -6 to 6
- b_up: float32 [57344, 2048], P(('expert', 'units')), parts along dimension 0, may hold values from -6 to 6
- b_down: float32 [57344, 2048], P(('expert', 'units')), parts along dimension 0, may hold values from -6 to 6
- perm: int32 [57344], P('expert'), parts along dimension 0, may hold values from 0 to 14335, as said below
Outputs:
- merged_up: float32 [57344, 2048], P(('expert', 'units')), parts along dimension 0
- merged_down: float32 [57344, 2048], P(('expert', 'units')), parts along dimension 0
The draws below stay inside these ranges and needn't reach their ends.
There are 4 independent parts, one for each index of `expert`. The reference program is written for one: setup_inputs(seed, part) draws one part's arguments, and reference() takes and returns one part's arrays. A program takes and returns all parts, laid end to end along the dimension named above; each array names one. Nothing has to cross between parts.
Inputs may be any that keep to these rules, and one draw needn't show every extreme that they name: perm names each of the 14336 units once. Cut the units into aligned blocks of 224: of the units of one source block, at most 5 are matched to units of any one destination block, and in every draw some pair of blocks reaches 5. Every source block sends the same list of counts to the destination blocks, in an order that differs from source to source.
All inputs are finite; a program needn't handle non-finite values.
Results may differ from the reference program's by a relative error of at most 0.00002.
Values sent between devices are 32-bit elements; how exact they have to be, the bound alone decides.
A program may use at most 64 MiB of HBM per device.

```python
import jax
import jax.numpy as jnp

FF = 14336
DW = 2048
CAP = 5
N_UNITS = 64


def draw_perm(key, part):
    per_dev = FF // N_UNITS
    count = N_UNITS
    limit = CAP
    keys = jax.random.split(jax.random.fold_in(key, 7), 6)
    spans = jax.random.randint(keys[0], (count,), limit - 1, limit + 1).astype(jnp.int32)
    spans = spans.at[0].set(limit)
    taken = jnp.cumsum(spans) - spans
    pieces = jnp.clip(per_dev - taken, 0, spans).astype(jnp.int32)
    ends = jnp.cumsum(pieces)
    slot = jnp.arange(per_dev, dtype=jnp.int32)
    which = jnp.sum((slot[:, None] >= ends[None, :]).astype(jnp.int32), axis=1)
    sigma = jax.random.permutation(keys[1], count).astype(jnp.int32)
    tau = jax.random.permutation(keys[2], count).astype(jnp.int32)
    sigma_inv = jnp.argsort(sigma).astype(jnp.int32)
    tau_inv = jnp.argsort(tau).astype(jnp.int32)
    source_order = jax.vmap(lambda subkey: jax.random.permutation(subkey, per_dev))(jax.random.split(keys[3], count)).astype(jnp.int32)
    target_order = jax.vmap(lambda subkey: jax.random.permutation(subkey, per_dev))(jax.random.split(keys[4], count)).astype(jnp.int32)
    dest = jnp.arange(count, dtype=jnp.int32)[:, None]
    source = tau_inv[(sigma_inv[dest] - which[None, :]) % count]
    dest_rows = dest * per_dev + target_order
    source_rows = source * per_dev + source_order[source, slot[None, :]]
    result = jnp.zeros((count * per_dev,), jnp.int32).at[dest_rows.reshape(-1)].set(source_rows.reshape(-1))
    return result


def shard_levels(key, shape, cuts, smallest, high):
    level = 1.0
    for axis_at, shards_of in cuts:
        steps = jax.random.uniform(jax.random.fold_in(jax.random.fold_in(key, 6), axis_at), (shards_of,), jnp.float32, smallest / len(cuts), high / len(cuts))
        level = level * jnp.repeat(jnp.exp(steps), shape[axis_at] // shards_of).reshape((-1,) + (1,) * (len(shape) - 1 - axis_at))
    return level


def bell_draw(stream_key, extent, deviation, reach, cuts=(), kind=jnp.bfloat16):
    array = jax.random.normal(stream_key, extent, jnp.float32) * deviation
    if len(cuts) > 0:
        array = shard_levels(stream_key, extent, cuts, -0.22, 0.18) * array
    return jnp.clip(array, min=-reach, max=reach).astype(kind)


def setup_inputs(seed: int = 0, part: int = 0) -> dict:
    key_of = jax.random.split(jax.random.key(seed), 6)
    own_keys = jax.random.split(jax.random.fold_in(key_of[5], part), 6)
    a_up = bell_draw(own_keys[0], (FF, DW), 1.0, 6.0, ((0, 64),), jnp.float32)
    a_down = bell_draw(own_keys[1], (FF, DW), 1.0, 6.0, ((0, 64),), jnp.float32)
    b_up = bell_draw(own_keys[2], (FF, DW), 1.0, 6.0, ((0, 64),), jnp.float32)
    b_down = bell_draw(own_keys[3], (FF, DW), 1.0, 6.0, ((0, 64),), jnp.float32)
    perm = draw_perm(jax.random.fold_in(jax.random.fold_in(key_of[5], part), 71), part)
    return {"a_up": a_up, "a_down": a_down, "b_up": b_up, "b_down": b_down, "perm": perm}


def reference(a_up, a_down, b_up, b_down, perm):
    permuted_up = jnp.take(b_up, perm, axis=0)
    permuted_down = jnp.take(b_down, perm, axis=0)
    merged_up = (a_up + permuted_up) * 0.5
    merged_down = (a_down + permuted_down) * 0.5
    return merged_up, merged_down
```

```python
import functools

import jax
import jax.numpy as jnp
from jax import lax
from jax.experimental import pallas as pl
from jax.experimental.pallas import tpu as pltpu
from jax.sharding import PartitionSpec as P

CAP = 5
LANES = 128
SUB = 8
CHUNK = SUB * LANES


def tables(perm, me, count, rows):
    grid = perm.reshape(count, rows)
    mine = grid // rows == me
    rank = jnp.cumsum(mine.astype(jnp.int32), axis=1) - 1
    local = grid - me * rows
    slots = [jnp.sum(jnp.where(mine & (rank == k), local, 0), axis=1) for k in range(CAP)]
    own = lax.dynamic_slice_in_dim(perm, me * rows, rows)
    source = own // rows
    place = jnp.arange(rows, dtype=jnp.int32)
    same = (source[None, :] == source[:, None]) & (place[None, :] < place[:, None])
    picks = source * CAP + jnp.sum(same.astype(jnp.int32), axis=1)
    return jnp.stack(slots, axis=1).reshape(-1), picks


def exchange(
    nx, nz, nc, chunks, slots, picks, a_up, a_down, b_up, b_down, o_up, o_down,
    a_buf, b_buf, o_buf, *rest
):
    sent = rest[:chunks]
    got = rest[chunks : 2 * chunks]
    in_sem, out_sem, send_sem, recv_sem = rest[2 * chunks :]
    count = nx * nz * nc
    rows, width = a_up.shape
    per = width // CHUNK
    me = lax.axis_index("units")
    mx, mz, mc = me // (nz * nc), me // nc % nz, me % nc

    def partner(t):
        dz, dx, dc = t // (nx * nc), t // nc % nx, t % nc
        return ((mx + dx) % nx * nz + (mz + dz) % nz) * nc + (mc + dc) % nc

    per_row = width // LANES

    def load(src, dst, sem):
        for k in range(per_row):
            pltpu.make_async_copy(src.at[:, pl.ds(k * LANES, LANES)], dst.at[:, k, :], sem).start()
        return pltpu.make_async_copy(dst, dst, sem)

    loads = [
        load(src, dst.at[m], in_sem.at[s])
        for s, (src, dst, m) in enumerate(
            ((b_up, b_buf, 0), (b_down, b_buf, 1), (a_up, a_buf, 0), (a_down, a_buf, 1))
        )
    ]
    barrier = pltpu.get_barrier_semaphore()

    @pl.loop(1, count)
    def _(t):
        pl.semaphore_signal(
            barrier, inc=1, device_id={"units": partner(t)}, device_id_type=pl.DeviceIdType.MESH
        )

    loads[0].wait()
    loads[1].wait()
    pl.semaphore_wait(barrier, count - 1)

    def pack(q, dest, into, where):
        m, at = q // per, q % per * SUB
        for r in range(CAP):
            into[where, r] = b_buf[m, slots[dest * CAP + r], at : at + SUB, :]

    for q in range(chunks):

        @pl.loop(1, count)
        def _(t):
            to = partner(t)
            pack(q, to, sent[q], t - 1)
            pltpu.make_async_remote_copy(
                src_ref=sent[q].at[t - 1],
                dst_ref=got[q].at[me],
                send_sem=send_sem.at[q],
                recv_sem=recv_sem.at[q],
                device_id={"units": to},
                device_id_type=pl.DeviceIdType.MESH,
            ).start()

        pack(q, me, got[q], me)

    loads[2].wait()
    loads[3].wait()
    outs = (o_up, o_down)
    stores = []
    for q in range(chunks):
        m, at = q // per, q % per * SUB
        every = pltpu.make_async_remote_copy(
            src_ref=sent[q],
            dst_ref=got[q].at[pl.ds(0, count - 1)],
            send_sem=send_sem.at[q],
            recv_sem=recv_sem.at[q],
            device_id={"units": me},
            device_id_type=pl.DeviceIdType.MESH,
        )
        every.wait_recv()

        @pl.loop(0, rows // SUB)
        def _(g):
            for s in range(SUB):
                j = g * SUB + s
                pick = picks[j]
                o_buf[q, j] = (a_buf[m, j, at : at + SUB, :] + got[q][pick // CAP, pick % CAP]) * 0.5

        for k in range(SUB):
            pltpu.make_async_copy(
                o_buf.at[q, :, k, :],
                outs[m].at[:, pl.ds((at + k) * LANES, LANES)],
                out_sem.at[q],
            ).start()
        stores.append(pltpu.make_async_copy(o_buf.at[q], o_buf.at[q], out_sem.at[q]))
        every.wait_send()
    for store in stores:
        store.wait()


def solution(mesh):
    nx, nz, nc = 4, 8, 2
    count = mesh.shape["units"]

    def on_device(a_up, a_down, b_up, b_down, perm):
        rows, width = a_up.shape
        me = lax.axis_index("units")
        slots, picks = tables(perm, me, count, rows)
        chunks = 2 * width // CHUNK
        shape = jax.ShapeDtypeStruct((rows, width), a_up.dtype)
        smem = pl.BlockSpec(memory_space=pltpu.SMEM)
        hbm = pl.BlockSpec(memory_space=pl.ANY)
        return pl.pallas_call(
            functools.partial(exchange, nx, nz, nc, chunks),
            out_shape=(shape, shape),
            in_specs=[smem, smem] + [hbm] * 4,
            out_specs=(hbm, hbm),
            scratch_shapes=[
                pltpu.VMEM((2, rows, width // LANES, LANES), jnp.float32),
                pltpu.VMEM((2, rows, width // LANES, LANES), jnp.float32),
                pltpu.VMEM((chunks, rows, SUB, LANES), jnp.float32),
                *[pltpu.VMEM((count - 1, CAP, SUB, LANES), jnp.float32)] * chunks,
                *[pltpu.VMEM((count, CAP, SUB, LANES), jnp.float32)] * chunks,
                pltpu.SemaphoreType.DMA((4,)),
                pltpu.SemaphoreType.DMA((chunks,)),
                pltpu.SemaphoreType.DMA((chunks,)),
                pltpu.SemaphoreType.DMA((chunks,)),
            ],
            compiler_params=pltpu.CompilerParams(
                collective_id=0, has_side_effects=True, vmem_limit_bytes=48 * 2**20
            ),
        )(slots, picks, a_up, a_down, b_up, b_down)

    units = P(("expert", "units"), None)
    return jax.shard_map(
        on_device,
        mesh=mesh,
        in_specs=(units, units, units, units, P("expert")),
        out_specs=(units, units),
        check_vma=False,
    )
```

```python
import functools

import jax
import jax.numpy as jnp
from jax import lax
from jax.experimental import pallas as pl
from jax.experimental.pallas import tpu as pltpu
from jax.sharding import PartitionSpec as P

CAP = 5
LANES = 128
SUB = 8
CHUNK = SUB * LANES
MESH = pl.DeviceIdType.MESH


def iota(shape, dim):
    return lax.broadcasted_iota(jnp.int32, shape, dim)


def strips(perm, groups, per_group):
    return [perm[pl.ds(r, groups, stride=per_group), :] for r in range(per_group)]


def slot_table(perm, table, me, rows, groups, per_group, per):
    lane = iota((groups, LANES), 1)
    left = []
    for strip in strips(perm, groups, per_group):
        local = strip - me * rows
        left.append(jnp.where((local >= 0) & (local < rows), local, -1))
    slots = jnp.zeros((groups, LANES), jnp.int32)
    for b in range(per):
        parts = []
        for r in range(b * rows // LANES, ((b + 1) * rows - 1) // LANES + 1):
            low, high = b * rows - r * LANES, (b + 1) * rows - r * LANES
            parts.append(jnp.where((lane >= low) & (lane < high), left[r], -1))
        for k in range(CAP):
            top = jnp.max(functools.reduce(jnp.maximum, parts), axis=1, keepdims=True)
            slots = jnp.where(lane == b * CAP + k, top, slots)
            parts = [jnp.where(part == top, -1, part) for part in parts]
    table[...] = jnp.maximum(slots, 0)


def pick_table(perm, table, me, rows, count, groups, per_group, per):
    group = me // per
    row = iota((SUB, LANES), 0)
    place = row * LANES + iota((SUB, LANES), 1)
    want = jnp.full((SUB, LANES), -1, jnp.int32)
    mine = iota((groups, LANES), 0) == group
    for r, strip in enumerate(strips(perm, groups, per_group)):
        line = jnp.max(jnp.where(mine, strip, -1), axis=0, keepdims=True)
        want = jnp.where(row == r, line, want)
    block = sum((place >= b * rows).astype(jnp.int32) for b in range(1, per))
    key = jnp.where(row < per_group, want + block * (count * rows), -1)
    whole = (key.astype(jnp.float32) + 0.5) * (1.0 / rows)
    source = whole.astype(jnp.int32)
    above = (source + 1) * rows

    def turn(s, ranks):
        for t in range(SUB):
            other = pltpu.roll(pltpu.roll(key, t, 0), s, 1)
            ranks = ranks + ((other > key) & (other < above)).astype(jnp.int32)
        return ranks

    ranks = lax.fori_loop(0, LANES, turn, jnp.zeros((SUB, LANES), jnp.int32))
    picks = (source - block * count) * CAP + ranks
    table[...] = jnp.clip(picks, 0, count * CAP - 1)


def exchange(nx, nz, nc, chunks, perm, a_up, a_down, b_up, b_down, *rest):
    merged, rest = rest[:chunks], rest[chunks:]
    sent, rest = rest[:chunks], rest[chunks:]
    got, rest = rest[:chunks], rest[chunks:]
    perm_buf, a_buf, b_one, b_two, slot_vmem, slots, pick_vmem, picks, in_sem, send_sem, recv_sem = rest
    count = nx * nz * nc
    rows, width = a_up.shape
    tiles = width // LANES
    half = tiles // SUB
    per = LANES * SUB // rows
    per_group = per * rows // LANES
    groups = count // per
    me = lax.axis_index("units")
    mx, mz, mc = me // (nz * nc), me // nc % nz, me % nc
    xs = [(mx + d) % nx * (nz * nc) for d in range(nx)]
    zs = [(mz + d) % nz * nc for d in range(nz)]
    cs = [(mc + d) % nc for d in range(nc)]

    barrier = pltpu.get_barrier_semaphore()
    for t in range(1, count):
        to = zs[t // (nx * nc)] + xs[t // nc % nx] + cs[t % nc]
        pl.semaphore_signal(barrier, inc=1, device_id={"units": to}, device_id_type=MESH)

    get_perm = pltpu.make_async_copy(perm, perm_buf, in_sem.at[4])
    get_perm.start()

    def load(src, dst, sem):
        for k in range(tiles):
            pltpu.make_async_copy(src.at[:, pl.ds(k * LANES, LANES)], dst.at[:, k, :], sem).start()
        return pltpu.make_async_copy(dst, dst, sem)

    loads = [
        load(src, dst, in_sem.at[s])
        for s, (src, dst) in enumerate(
            ((b_up, b_one), (b_down, b_two), (a_up, a_buf.at[0]), (a_down, a_buf.at[1]))
        )
    ]
    get_perm.wait()
    slot_table(perm_buf, slot_vmem, me, rows, groups, per_group, per)
    to_smem = pltpu.make_async_copy(slot_vmem, slots, in_sem.at[5])
    to_smem.start()
    to_smem.wait()

    def partner(t):
        dz, dx, dc = t // (nx * nc), t // nc % nx, t % nc
        return ((mx + dx) % nx * nz + (mz + dz) % nz) * nc + (mc + dc) % nc

    def pack(q, dest, into, where):
        b_buf, at = (b_one, b_two)[q // half], q % half * SUB
        for r in range(CAP):
            into[where + r] = b_buf[slots[dest // per, dest % per * CAP + r], at : at + SUB, :]

    for q in range(chunks):
        if q % half == 0:
            loads[q // half].wait()

        @pl.loop(1, count)
        def _(t):
            pack(q, partner(t), sent[q], (t - 1) * CAP)

        pack(q, me, got[q], me * CAP)
        if q == 0:
            pl.semaphore_wait(barrier, count - 1)

        @pl.loop(1, count)
        def _(t):
            pltpu.make_async_remote_copy(
                src_ref=sent[q].at[pl.ds((t - 1) * CAP, CAP)],
                dst_ref=got[q].at[pl.ds(me * CAP, CAP)],
                send_sem=send_sem.at[q],
                recv_sem=recv_sem.at[q],
                device_id={"units": partner(t)},
                device_id_type=MESH,
            ).start()

    pick_table(perm_buf, pick_vmem, me, rows, count, groups, per_group, per)
    to_smem = pltpu.make_async_copy(pick_vmem, picks, in_sem.at[5])
    to_smem.start()
    to_smem.wait()
    first = me % per * rows
    loads[2].wait()
    loads[3].wait()
    for q in range(chunks):
        m, at = q // half, q % half * SUB
        every = pltpu.make_async_remote_copy(
            src_ref=sent[q],
            dst_ref=got[q].at[pl.ds(0, (count - 1) * CAP)],
            send_sem=send_sem.at[q],
            recv_sem=recv_sem.at[q],
            device_id={"units": me},
            device_id_type=MESH,
        )
        every.wait_recv()

        @pl.loop(0, rows // SUB)
        def _(g):
            for s in range(SUB):
                j = g * SUB + s
                e = first + j
                pick = picks[e // LANES, e % LANES]
                merged[q][j] = (a_buf[m, j, at : at + SUB, :] + got[q][pick]) * 0.5

        every.wait_send()


def write_out(chunks, *refs):
    merged, outs, sem = refs[:chunks], refs[chunks:-1], refs[-1]
    half = chunks // 2
    for q in range(chunks):
        for k in range(SUB):
            column = (q % half * SUB + k) * LANES
            pltpu.make_async_copy(
                merged[q].at[:, k, :], outs[q // half].at[:, pl.ds(column, LANES)], sem.at[q]
            ).start()
    for q in range(chunks):
        pltpu.make_async_copy(merged[q], merged[q], sem.at[q]).wait()


def solution(mesh):
    nx, nz, nc = 4, 8, 2
    count = mesh.shape["units"]

    def on_device(a_up, a_down, b_up, b_down, perm):
        rows, width = a_up.shape
        chunks = 2 * width // CHUNK
        hbm = pl.BlockSpec(memory_space=pltpu.HBM)
        vmem = pl.BlockSpec(memory_space=pltpu.VMEM)
        merged = pl.pallas_call(
            functools.partial(exchange, nx, nz, nc, chunks),
            out_shape=[pltpu.VMEM((rows, SUB, LANES), jnp.float32)] * chunks,
            in_specs=[hbm] * 5,
            out_specs=[vmem] * chunks,
            scratch_shapes=[
                *[pltpu.VMEM(((count - 1) * CAP, SUB, LANES), jnp.float32)] * chunks,
                *[pltpu.VMEM((count * CAP, SUB, LANES), jnp.float32)] * chunks,
                pltpu.VMEM((perm.shape[0] // LANES, LANES), jnp.int32),
                pltpu.VMEM((2, rows, width // LANES, LANES), jnp.float32),
                pltpu.VMEM((rows, width // LANES, LANES), jnp.float32),
                pltpu.VMEM((rows, width // LANES, LANES), jnp.float32),
                pltpu.VMEM((count // (CHUNK // rows), LANES), jnp.int32),
                pltpu.SMEM((count // (CHUNK // rows), LANES), jnp.int32),
                pltpu.VMEM((SUB, LANES), jnp.int32),
                pltpu.SMEM((SUB, LANES), jnp.int32),
                pltpu.SemaphoreType.DMA((6,)),
                pltpu.SemaphoreType.DMA((chunks,)),
                pltpu.SemaphoreType.DMA((chunks,)),
            ],
            compiler_params=pltpu.CompilerParams(
                collective_id=0, has_side_effects=True, vmem_limit_bytes=59 * 2**20
            ),
        )(perm.reshape(-1, LANES), a_up, a_down, b_up, b_down)
        shape = jax.ShapeDtypeStruct((rows, width), jnp.float32)
        return pl.pallas_call(
            functools.partial(write_out, chunks),
            out_shape=(shape, shape),
            in_specs=[pl.BlockSpec(memory_space=pl.ANY)] * chunks,
            out_specs=(hbm, hbm),
            scratch_shapes=[pltpu.SemaphoreType.DMA((chunks,))],
            compiler_params=pltpu.CompilerParams(vmem_limit_bytes=2**20),
        )(*merged)

    units = P(("expert", "units"), None)
    return jax.shard_map(
        on_device,
        mesh=mesh,
        in_specs=(units, units, units, units, P("expert")),
        out_specs=(units, units),
        check_vma=False,
    )
```

```python
import functools

import jax
import jax.numpy as jnp
from jax import lax
from jax.experimental import pallas as pl
from jax.experimental.pallas import tpu as pltpu
from jax.sharding import PartitionSpec as P

CAP = 5
LANES = 128
SUB = 8
CHUNK = SUB * LANES
STEP = 16
Z_ORDER = (4, 3, 5, 2, 6, 1, 7, 0)
MESH = pl.DeviceIdType.MESH


def iota(shape, dim):
    return lax.broadcasted_iota(jnp.int32, shape, dim)


def strips(perm, groups, per_group):
    return [perm[pl.ds(r, groups, stride=per_group), :] for r in range(per_group)]


def slot_table(perm, table, me, rows, groups, per_group, per):
    lane = iota((groups, LANES), 1)
    left = []
    for strip in strips(perm, groups, per_group):
        local = strip - me * rows
        left.append(jnp.where((local >= 0) & (local < rows), local, -1))
    slots = jnp.zeros((groups, LANES), jnp.int32)
    for b in range(per):
        parts = []
        for r in range(b * rows // LANES, ((b + 1) * rows - 1) // LANES + 1):
            low, high = b * rows - r * LANES, (b + 1) * rows - r * LANES
            parts.append(jnp.where((lane >= low) & (lane < high), left[r], -1))
        for k in range(CAP):
            top = jnp.max(functools.reduce(jnp.maximum, parts), axis=1, keepdims=True)
            slots = jnp.where(lane == b * CAP + k, top, slots)
            parts = [jnp.where(part == top, -1, part) for part in parts]
    table[...] = jnp.maximum(slots, 0)


def pick_table(perm, table, me, rows, count, groups, per_group, per):
    group = me // per
    row = iota((SUB, LANES), 0)
    place = row * LANES + iota((SUB, LANES), 1)
    want = jnp.full((SUB, LANES), -1, jnp.int32)
    mine = iota((groups, LANES), 0) == group
    for r, strip in enumerate(strips(perm, groups, per_group)):
        line = jnp.max(jnp.where(mine, strip, -1), axis=0, keepdims=True)
        want = jnp.where(row == r, line, want)
    block = sum((place >= b * rows).astype(jnp.int32) for b in range(1, per))
    key = jnp.where(row < per_group, want + block * (count * rows), -1)
    whole = (key.astype(jnp.float32) + 0.5) * (1.0 / rows)
    source = whole.astype(jnp.int32)
    above = (source + 1) * rows

    def turn(s, ranks):
        for t in range(SUB):
            other = pltpu.roll(pltpu.roll(key, t, 0), s, 1)
            ranks = ranks + ((other > key) & (other < above)).astype(jnp.int32)
        return ranks

    ranks = lax.fori_loop(0, LANES, turn, jnp.zeros((SUB, LANES), jnp.int32))
    picks = (source - block * count) * CAP + ranks
    table[...] = jnp.clip(picks, 0, count * CAP - 1)


def exchange(nx, nz, nc, chunks, perm, a_up, a_down, b_up, b_down, *rest):
    merged, rest = rest[:chunks], rest[chunks:]
    sent, rest = rest[:chunks], rest[chunks:]
    got, rest = rest[:chunks], rest[chunks:]
    perm_buf, a_buf, b_one, b_two, slot_vmem, slots, pick_vmem, picks, own_picks, in_sem, send_sem, recv_sem = rest
    count = nx * nz * nc
    rows, width = a_up.shape
    tiles = width // LANES
    half = tiles // SUB
    per = LANES * SUB // rows
    per_group = per * rows // LANES
    groups = count // per
    me = lax.axis_index("units")
    mx, mz, mc = me // (nz * nc), me // nc % nz, me % nc
    xs = [(mx + d) % nx * (nz * nc) for d in range(nx)]
    zs = [(mz + d) % nz * nc for d in range(nz)]
    cs = [(mc + d) % nc for d in range(nc)]

    get_perm = pltpu.make_async_copy(perm, perm_buf, in_sem.at[4])
    get_perm.start()
    barrier = pltpu.get_barrier_semaphore()
    for dz in Z_ORDER:
        for u in range(dz == 0, nx * nc):
            to = zs[dz] + xs[u // nc] + cs[u % nc]
            pl.semaphore_signal(barrier, inc=1, device_id={"units": to}, device_id_type=MESH)

    def load(src, dst, sem):
        for k in range(tiles):
            pltpu.make_async_copy(src.at[:, pl.ds(k * LANES, LANES)], dst.at[:, k, :], sem).start()
        return pltpu.make_async_copy(dst, dst, sem)

    loads = [load(b_up, b_one, in_sem.at[0])]
    get_perm.wait()
    slot_table(perm_buf, slot_vmem, me, rows, groups, per_group, per)
    to_smem = pltpu.make_async_copy(slot_vmem, slots, in_sem.at[5])
    to_smem.start()
    to_smem.wait()

    def pack(q, at_slots, into):
        b_buf, at = (b_one, b_two)[q // half], q % half * SUB
        values = [b_buf[i, at : at + SUB, :] for i in at_slots]
        for r, value in enumerate(values):
            into(r)[...] = value

    def send(q, to):
        pltpu.make_async_remote_copy(
            src_ref=sent[q].at[pl.ds(to * CAP, CAP)],
            dst_ref=got[q].at[pl.ds(me * CAP, CAP)],
            send_sem=send_sem.at[q],
            recv_sem=recv_sem.at[q],
            device_id={"units": to},
            device_id_type=MESH,
        ).start()

    for q in range(chunks):
        if q % half == 0:
            loads[q // half].wait()

        @pl.loop(0, groups)
        def _(g):
            for b in range(0, per, 2):
                pack(
                    q,
                    [slots[g, b * CAP + r] for r in range(2 * CAP)],
                    lambda r: sent[q].at[(g * per + b) * CAP + r],
                )

        if q == 0:
            pl.semaphore_wait(barrier, count - 1)
        for dz in Z_ORDER:
            if q == 0:
                for u in range(dz == 0, nx * nc):
                    send(q, zs[dz] + xs[u // nc] + cs[u % nc])
            else:

                @pl.loop(int(dz == 0), nx * nc)
                def _(u):
                    send(q, zs[dz] + (mx + u // nc) % nx * (nz * nc) + (mc + u % nc) % nc)

        if q == 0:
            loads.append(load(b_down, b_two, in_sem.at[1]))
            loads.append(load(a_up, a_buf.at[0], in_sem.at[2]))
            loads.append(load(a_down, a_buf.at[1], in_sem.at[3]))
        pack(
            q,
            [slots[me // per, me % per * CAP + r] for r in range(CAP)],
            lambda r: got[q].at[me * CAP + r],
        )

    pick_table(perm_buf, pick_vmem, me, rows, count, groups, per_group, per)
    to_smem = pltpu.make_async_copy(pick_vmem, picks, in_sem.at[5])
    to_smem.start()
    to_smem.wait()
    first = me % per * rows

    @pl.loop(0, rows)
    def _(j):
        own_picks[j] = picks[(first + j) // LANES, (first + j) % LANES]

    loads[2].wait()
    loads[3].wait()
    for q in range(chunks):
        m, at = q // half, q % half * SUB
        every = pltpu.make_async_remote_copy(
            src_ref=sent[q].at[pl.ds(0, (count - 1) * CAP)],
            dst_ref=got[q].at[pl.ds(0, (count - 1) * CAP)],
            send_sem=send_sem.at[q],
            recv_sem=recv_sem.at[q],
            device_id={"units": me},
            device_id_type=MESH,
        )
        every.wait_recv()

        @pl.loop(0, rows // STEP)
        def _(g):
            sums = [
                a_buf[m, g * STEP + s, at : at + SUB, :] + got[q][own_picks[g * STEP + s]]
                for s in range(STEP)
            ]
            for s, value in enumerate(sums):
                merged[q][g * STEP + s] = value * 0.5

        every.wait_send()


def write_out(chunks, *refs):
    merged, outs, sem = refs[:chunks], refs[chunks:-1], refs[-1]
    half = chunks // 2
    for q in range(chunks):
        for k in range(SUB):
            column = (q % half * SUB + k) * LANES
            pltpu.make_async_copy(
                merged[q].at[:, k, :], outs[q // half].at[:, pl.ds(column, LANES)], sem.at[q]
            ).start()
    for q in range(chunks):
        pltpu.make_async_copy(merged[q], merged[q], sem.at[q]).wait()


def solution(mesh):
    nx, nz, nc = 4, 8, 2
    count = mesh.shape["units"]

    def on_device(a_up, a_down, b_up, b_down, perm):
        rows, width = a_up.shape
        chunks = 2 * width // CHUNK
        hbm = pl.BlockSpec(memory_space=pltpu.HBM)
        vmem = pl.BlockSpec(memory_space=pltpu.VMEM)
        merged = pl.pallas_call(
            functools.partial(exchange, nx, nz, nc, chunks),
            out_shape=[pltpu.VMEM((rows, SUB, LANES), jnp.float32)] * chunks,
            in_specs=[hbm] * 5,
            out_specs=[vmem] * chunks,
            scratch_shapes=[
                *[pltpu.VMEM((count * CAP, SUB, LANES), jnp.float32)] * chunks,
                *[pltpu.VMEM((count * CAP, SUB, LANES), jnp.float32)] * chunks,
                pltpu.VMEM((perm.shape[0] // LANES, LANES), jnp.int32),
                pltpu.VMEM((2, rows, width // LANES, LANES), jnp.float32),
                pltpu.VMEM((rows, width // LANES, LANES), jnp.float32),
                pltpu.VMEM((rows, width // LANES, LANES), jnp.float32),
                pltpu.VMEM((count // (CHUNK // rows), LANES), jnp.int32),
                pltpu.SMEM((count // (CHUNK // rows), LANES), jnp.int32),
                pltpu.VMEM((SUB, LANES), jnp.int32),
                pltpu.SMEM((SUB, LANES), jnp.int32),
                pltpu.SMEM((rows,), jnp.int32),
                pltpu.SemaphoreType.DMA((6,)),
                pltpu.SemaphoreType.DMA((chunks,)),
                pltpu.SemaphoreType.DMA((chunks,)),
            ],
            compiler_params=pltpu.CompilerParams(
                collective_id=0, has_side_effects=True, vmem_limit_bytes=59 * 2**20
            ),
        )(perm.reshape(-1, LANES), a_up, a_down, b_up, b_down)
        shape = jax.ShapeDtypeStruct((rows, width), jnp.float32)
        return pl.pallas_call(
            functools.partial(write_out, chunks),
            out_shape=(shape, shape),
            in_specs=[pl.BlockSpec(memory_space=pl.ANY)] * chunks,
            out_specs=(hbm, hbm),
            scratch_shapes=[pltpu.SemaphoreType.DMA((chunks,))],
            compiler_params=pltpu.CompilerParams(vmem_limit_bytes=2**20),
        )(*merged)

    units = P(("expert", "units"), None)
    return jax.shard_map(
        on_device,
        mesh=mesh,
        in_specs=(units, units, units, units, P("expert")),
        out_specs=(units, units),
        check_vma=False,
    )
```

```python
import functools

import jax
import jax.numpy as jnp
from jax import lax
from jax.experimental import pallas as pl
from jax.experimental.pallas import tpu as pltpu
from jax.sharding import PartitionSpec as P

CAP = 5
LANES = 128
SUB = 8
CHUNK = SUB * LANES
STEP = 16
Z_ORDER = (4, 3, 5, 2, 6, 1, 7, 0)
MESH = pl.DeviceIdType.MESH


def iota(shape, dim):
    return lax.broadcasted_iota(jnp.int32, shape, dim)


def strips(perm, groups, per_group):
    return [perm[pl.ds(r, groups, stride=per_group), :] for r in range(per_group)]


def slot_table(perm, table, me, rows, groups, per_group, per):
    lane = iota((groups, LANES), 1)
    left = []
    for strip in strips(perm, groups, per_group):
        local = strip - me * rows
        left.append(jnp.where((local >= 0) & (local < rows), local, -1))
    slots = jnp.zeros((groups, LANES), jnp.int32)
    for b in range(per):
        parts = []
        for r in range(b * rows // LANES, ((b + 1) * rows - 1) // LANES + 1):
            low, high = b * rows - r * LANES, (b + 1) * rows - r * LANES
            parts.append(jnp.where((lane >= low) & (lane < high), left[r], -1))
        for k in range(CAP):
            top = jnp.max(functools.reduce(jnp.maximum, parts), axis=1, keepdims=True)
            slots = jnp.where(lane == b * CAP + k, top, slots)
            parts = [jnp.where(part == top, -1, part) for part in parts]
    table[...] = jnp.maximum(slots, 0)


def pick_table(perm, table, me, rows, count, groups, per_group, per):
    group = me // per
    row = iota((SUB, LANES), 0)
    place = row * LANES + iota((SUB, LANES), 1)
    want = jnp.full((SUB, LANES), -1, jnp.int32)
    mine = iota((groups, LANES), 0) == group
    for r, strip in enumerate(strips(perm, groups, per_group)):
        line = jnp.max(jnp.where(mine, strip, -1), axis=0, keepdims=True)
        want = jnp.where(row == r, line, want)
    block = sum((place >= b * rows).astype(jnp.int32) for b in range(1, per))
    key = jnp.where(row < per_group, want + block * (count * rows), -1)
    whole = (key.astype(jnp.float32) + 0.5) * (1.0 / rows)
    source = whole.astype(jnp.int32)
    above = (source + 1) * rows

    def turn(s, ranks):
        for t in range(SUB):
            other = pltpu.roll(pltpu.roll(key, t, 0), s, 1)
            ranks = ranks + ((other > key) & (other < above)).astype(jnp.int32)
        return ranks

    ranks = lax.fori_loop(0, LANES, turn, jnp.zeros((SUB, LANES), jnp.int32))
    picks = (source - block * count) * CAP + ranks
    table[...] = jnp.clip(picks, 0, count * CAP - 1)


def exchange(nx, nz, nc, chunks, perm, a_up, a_down, b_up, b_down, *rest):
    merged, rest = rest[:chunks], rest[chunks:]
    sent, rest = rest[:chunks], rest[chunks:]
    got, rest = rest[:chunks], rest[chunks:]
    perm_buf, a_buf, b_one, b_two, slot_vmem, slots, pick_vmem, picks, own_picks, heard, in_sem, send_sem, recv_sem = rest
    count = nx * nz * nc
    rows, width = a_up.shape
    tiles = width // LANES
    half = tiles // SUB
    per = LANES * SUB // rows
    per_group = per * rows // LANES
    groups = count // per
    me = lax.axis_index("units")
    mx, mz, mc = me // (nz * nc), me // nc % nz, me % nc
    xs = [(mx + d) % nx * (nz * nc) for d in range(nx)]
    zs = [(mz + d) % nz * nc for d in range(nz)]
    cs = [(mc + d) % nc for d in range(nc)]

    get_perm = pltpu.make_async_copy(perm, perm_buf, in_sem.at[4])
    get_perm.start()
    barrier = pltpu.get_barrier_semaphore()
    near = [(dz, u) for dz in (1, nz - 1, 0) for u in range(dz == 0, nx * nc)]
    for dz, u in near:
        pl.semaphore_signal(
            barrier,
            inc=1,
            device_id={"units": zs[dz] + xs[u // nc] + cs[u % nc]},
            device_id_type=MESH,
        )

    def tell(k, dz):
        pl.semaphore_signal(
            heard.at[k], inc=1, device_id={"units": zs[dz] + xs[0] + cs[0]}, device_id_type=MESH
        )

    def load(src, dst, sem):
        for k in range(tiles):
            pltpu.make_async_copy(src.at[:, pl.ds(k * LANES, LANES)], dst.at[:, k, :], sem).start()
        return pltpu.make_async_copy(dst, dst, sem)

    loads = [load(b_up, b_one, in_sem.at[0])]
    get_perm.wait()
    slot_table(perm_buf, slot_vmem, me, rows, groups, per_group, per)
    to_smem = pltpu.make_async_copy(slot_vmem, slots, in_sem.at[5])
    to_smem.start()
    pl.semaphore_wait(barrier, len(near))
    tell(0, 1)
    tell(1, nz - 1)
    to_smem.wait()

    def pack(q, at_slots, into):
        b_buf, at = (b_one, b_two)[q // half], q % half * SUB
        values = [b_buf[i, at : at + SUB, :] for i in at_slots]
        for r, value in enumerate(values):
            into(r)[...] = value

    def send(q, to):
        pltpu.make_async_remote_copy(
            src_ref=sent[q].at[pl.ds(to * CAP, CAP)],
            dst_ref=got[q].at[pl.ds(me * CAP, CAP)],
            send_sem=send_sem.at[q],
            recv_sem=recv_sem.at[q],
            device_id={"units": to},
            device_id_type=MESH,
        ).start()

    for q in range(chunks):
        if q % half == 0:
            loads[q // half].wait()

        @pl.loop(0, groups)
        def _(g):
            for b in range(0, per, 2):
                pack(
                    q,
                    [slots[g, b * CAP + r] for r in range(2 * CAP)],
                    lambda r: sent[q].at[(g * per + b) * CAP + r],
                )

        if q == 0:
            for dz, u in near:
                send(q, zs[dz] + xs[u // nc] + cs[u % nc])
            for step in range(2, nz // 2 + 1):
                pl.semaphore_wait(heard.at[2 * step - 4], 1)
                if step < nz // 2:
                    tell(2 * step - 2, 1)
                    pl.semaphore_wait(heard.at[2 * step - 3], 1)
                    if step + 1 < nz // 2:
                        tell(2 * step - 1, nz - 1)
                for dz in sorted({step, nz - step}):
                    for u in range(nx * nc):
                        send(q, zs[dz] + xs[u // nc] + cs[u % nc])
        else:
            for dz in Z_ORDER:

                @pl.loop(int(dz == 0), nx * nc)
                def _(u):
                    send(q, zs[dz] + (mx + u // nc) % nx * (nz * nc) + (mc + u % nc) % nc)

        if q == 0:
            loads.append(load(b_down, b_two, in_sem.at[1]))
            loads.append(load(a_up, a_buf.at[0], in_sem.at[2]))
            loads.append(load(a_down, a_buf.at[1], in_sem.at[3]))
        pack(
            q,
            [slots[me // per, me % per * CAP + r] for r in range(CAP)],
            lambda r: got[q].at[me * CAP + r],
        )

    pick_table(perm_buf, pick_vmem, me, rows, count, groups, per_group, per)
    to_smem = pltpu.make_async_copy(pick_vmem, picks, in_sem.at[5])
    to_smem.start()
    to_smem.wait()
    first = me % per * rows

    @pl.loop(0, rows)
    def _(j):
        own_picks[j] = picks[(first + j) // LANES, (first + j) % LANES]

    loads[2].wait()
    loads[3].wait()
    for q in range(chunks):
        m, at = q // half, q % half * SUB
        every = pltpu.make_async_remote_copy(
            src_ref=sent[q].at[pl.ds(0, (count - 1) * CAP)],
            dst_ref=got[q].at[pl.ds(0, (count - 1) * CAP)],
            send_sem=send_sem.at[q],
            recv_sem=recv_sem.at[q],
            device_id={"units": me},
            device_id_type=MESH,
        )
        every.wait_recv()

        @pl.loop(0, rows // STEP)
        def _(g):
            sums = [
                a_buf[m, g * STEP + s, at : at + SUB, :] + got[q][own_picks[g * STEP + s]]
                for s in range(STEP)
            ]
            for s, value in enumerate(sums):
                merged[q][g * STEP + s] = value * 0.5

        every.wait_send()


def write_out(chunks, *refs):
    merged, outs, sem = refs[:chunks], refs[chunks:-1], refs[-1]
    half = chunks // 2
    for q in range(chunks):
        for k in range(SUB):
            column = (q % half * SUB + k) * LANES
            pltpu.make_async_copy(
                merged[q].at[:, k, :], outs[q // half].at[:, pl.ds(column, LANES)], sem.at[q]
            ).start()
    for q in range(chunks):
        pltpu.make_async_copy(merged[q], merged[q], sem.at[q]).wait()


def solution(mesh):
    nx, nz, nc = 4, 8, 2
    count = mesh.shape["units"]

    def on_device(a_up, a_down, b_up, b_down, perm):
        rows, width = a_up.shape
        chunks = 2 * width // CHUNK
        hbm = pl.BlockSpec(memory_space=pltpu.HBM)
        vmem = pl.BlockSpec(memory_space=pltpu.VMEM)
        merged = pl.pallas_call(
            functools.partial(exchange, nx, nz, nc, chunks),
            out_shape=[pltpu.VMEM((rows, SUB, LANES), jnp.float32)] * chunks,
            in_specs=[hbm] * 5,
            out_specs=[vmem] * chunks,
            scratch_shapes=[
                *[pltpu.VMEM((count * CAP, SUB, LANES), jnp.float32)] * chunks,
                *[pltpu.VMEM((count * CAP, SUB, LANES), jnp.float32)] * chunks,
                pltpu.VMEM((perm.shape[0] // LANES, LANES), jnp.int32),
                pltpu.VMEM((2, rows, width // LANES, LANES), jnp.float32),
                pltpu.VMEM((rows, width // LANES, LANES), jnp.float32),
                pltpu.VMEM((rows, width // LANES, LANES), jnp.float32),
                pltpu.VMEM((count // (CHUNK // rows), LANES), jnp.int32),
                pltpu.SMEM((count // (CHUNK // rows), LANES), jnp.int32),
                pltpu.VMEM((SUB, LANES), jnp.int32),
                pltpu.SMEM((SUB, LANES), jnp.int32),
                pltpu.SMEM((rows,), jnp.int32),
                pltpu.SemaphoreType.REGULAR((nz - 3,)),
                pltpu.SemaphoreType.DMA((6,)),
                pltpu.SemaphoreType.DMA((chunks,)),
                pltpu.SemaphoreType.DMA((chunks,)),
            ],
            compiler_params=pltpu.CompilerParams(
                collective_id=0, has_side_effects=True, vmem_limit_bytes=59 * 2**20
            ),
        )(perm.reshape(-1, LANES), a_up, a_down, b_up, b_down)
        shape = jax.ShapeDtypeStruct((rows, width), jnp.float32)
        return pl.pallas_call(
            functools.partial(write_out, chunks),
            out_shape=(shape, shape),
            in_specs=[pl.BlockSpec(memory_space=pl.ANY)] * chunks,
            out_specs=(hbm, hbm),
            scratch_shapes=[pltpu.SemaphoreType.DMA((chunks,))],
            compiler_params=pltpu.CompilerParams(vmem_limit_bytes=2**20),
        )(*merged)

    units = P(("expert", "units"), None)
    return jax.shard_map(
        on_device,
        mesh=mesh,
        in_specs=(units, units, units, units, P("expert")),
        out_specs=(units, units),
        check_vma=False,
    )
```

```python
import functools

import jax
import jax.numpy as jnp
from jax import lax
from jax.experimental import pallas as pl
from jax.experimental.pallas import tpu as pltpu
from jax.sharding import PartitionSpec as P

CAP = 5
LANES = 128
SUB = 8
CHUNK = SUB * LANES
STEP = 16
Z_ORDER = (0, 4, 3, 5, 2, 6, 1, 7)
PLANES = (0, 4, 1, 5, 2, 6, 3, 7)
MESH = pl.DeviceIdType.MESH


def iota(shape, dim):
    return lax.broadcasted_iota(jnp.int32, shape, dim)


def strips(perm, groups, per_group):
    return [perm[pl.ds(r, groups, stride=per_group), :] for r in range(per_group)]


def slot_table(perm, table, me, rows, groups, per_group, per):
    lane = iota((groups, LANES), 1)
    left = []
    for strip in strips(perm, groups, per_group):
        local = strip - me * rows
        left.append(jnp.where((local >= 0) & (local < rows), local, -1))
    slots = jnp.zeros((groups, LANES), jnp.int32)
    for b in range(per):
        parts = []
        for r in range(b * rows // LANES, ((b + 1) * rows - 1) // LANES + 1):
            low, high = b * rows - r * LANES, (b + 1) * rows - r * LANES
            parts.append(jnp.where((lane >= low) & (lane < high), left[r], -1))
        for k in range(CAP):
            top = jnp.max(functools.reduce(jnp.maximum, parts), axis=1, keepdims=True)
            slots = jnp.where(lane == b * CAP + k, top, slots)
            parts = [jnp.where(part == top, -1, part) for part in parts]
    table[...] = jnp.maximum(slots, 0)


def pick_table(perm, table, me, rows, count, groups, per_group, per):
    group = me // per
    row = iota((SUB, LANES), 0)
    place = row * LANES + iota((SUB, LANES), 1)
    want = jnp.full((SUB, LANES), -1, jnp.int32)
    mine = iota((groups, LANES), 0) == group
    for r, strip in enumerate(strips(perm, groups, per_group)):
        line = jnp.max(jnp.where(mine, strip, -1), axis=0, keepdims=True)
        want = jnp.where(row == r, line, want)
    block = sum((place >= b * rows).astype(jnp.int32) for b in range(1, per))
    key = jnp.where(row < per_group, want + block * (count * rows), -1)
    whole = (key.astype(jnp.float32) + 0.5) * (1.0 / rows)
    source = whole.astype(jnp.int32)
    above = (source + 1) * rows

    def turn(s, ranks):
        for t in range(SUB):
            other = pltpu.roll(pltpu.roll(key, t, 0), s, 1)
            ranks = ranks + ((other > key) & (other < above)).astype(jnp.int32)
        return ranks

    ranks = lax.fori_loop(0, LANES, turn, jnp.zeros((SUB, LANES), jnp.int32))
    picks = (source - block * count) * CAP + ranks
    table[...] = jnp.clip(picks, 0, count * CAP - 1)


def exchange(nx, nz, nc, chunks, perm, a_up, a_down, b_up, b_down, *rest):
    merged, rest = rest[:chunks], rest[chunks:]
    sent, rest = rest[:chunks], rest[chunks:]
    got, rest = rest[:chunks], rest[chunks:]
    b_bufs, rest = rest[:chunks], rest[chunks:]
    perm_buf, a_buf, slot_vmem, slots, pick_vmem, picks, own_picks, heard, *sems = rest
    in_sem, b_sem, send_sem, recv_sem = sems
    count = nx * nz * nc
    rows, width = a_up.shape
    tiles = width // LANES
    half = tiles // SUB
    per = LANES * SUB // rows
    per_group = per * rows // LANES
    groups = count // per
    me = lax.axis_index("units")
    mx, mz, mc = lax.div(me, nz * nc), lax.rem(lax.div(me, nc), nz), lax.rem(me, nc)
    xs = [lax.rem(mx + d, nx) * (nz * nc) for d in range(nx)]
    zs = [lax.rem(mz + d, nz) * nc for d in range(nz)]
    cs = [lax.rem(mc + d, nc) for d in range(nc)]

    get_perm = pltpu.make_async_copy(perm, perm_buf, in_sem.at[2])
    get_perm.start()

    def load(src, column, dst, sem):
        for k in range(dst.shape[1]):
            pltpu.make_async_copy(
                src.at[:, pl.ds(column + k * LANES, LANES)], dst.at[:, k, :], sem
            ).start()
        return pltpu.make_async_copy(dst, dst, sem)

    def load_b(q):
        return load((b_up, b_down)[q // half], q % half * CHUNK, b_bufs[q], b_sem.at[q])

    b_loads = [load_b(0)]
    barrier = pltpu.get_barrier_semaphore()
    near = [(dz, u) for dz in (1, nz - 1, 0) for u in range(dz == 0, nx * nc)]
    for dz, u in near:
        pl.semaphore_signal(
            barrier,
            inc=1,
            device_id={"units": zs[dz] + xs[u // nc] + cs[u % nc]},
            device_id_type=MESH,
        )

    def tell(k, dz):
        pl.semaphore_signal(
            heard.at[k], inc=1, device_id={"units": zs[dz] + xs[0] + cs[0]}, device_id_type=MESH
        )

    get_perm.wait()
    slot_table(perm_buf, slot_vmem, me, rows, groups, per_group, per)
    to_smem = pltpu.make_async_copy(slot_vmem, slots, in_sem.at[3])
    to_smem.start()
    pl.semaphore_wait(barrier, len(near))
    tell(0, 1)
    tell(1, nz - 1)
    to_smem.wait()

    def pack(q, at_slots, into):
        values = [b_bufs[q][i] for i in at_slots]
        for r, value in enumerate(values):
            into(r)[...] = value

    def send(q, to):
        pltpu.make_async_remote_copy(
            src_ref=sent[q].at[pl.ds(to * CAP, CAP)],
            dst_ref=got[q].at[pl.ds(me * CAP, CAP)],
            send_sem=send_sem.at[q],
            recv_sem=recv_sem.at[q],
            device_id={"units": to},
            device_id_type=MESH,
        ).start()

    for q in range(chunks):
        b_loads[q].wait()

        @pl.loop(0, groups)
        def _(g):
            for b in range(0, per, 2):
                pack(
                    q,
                    [slots[g, b * CAP + r] for r in range(2 * CAP)],
                    lambda r: sent[q].at[(g * per + b) * CAP + r],
                )

        if q == 0:
            for dz, u in near:
                send(q, zs[dz] + xs[u // nc] + cs[u % nc])
            for step in range(2, nz // 2 + 1):
                pl.semaphore_wait(heard.at[2 * step - 4], 1)
                if step < nz // 2:
                    tell(2 * step - 2, 1)
                    pl.semaphore_wait(heard.at[2 * step - 3], 1)
                    if step + 1 < nz // 2:
                        tell(2 * step - 1, nz - 1)
                for dz in sorted({step, nz - step}):
                    for u in range(nx * nc):
                        send(q, zs[dz] + xs[u // nc] + cs[u % nc])
        elif q < chunks - 1:
            for dz in Z_ORDER:

                @pl.loop(int(dz == 0), nx * nc)
                def _(u):
                    x = lax.rem(mx + lax.div(u, nc), nx)
                    send(q, zs[dz] + x * (nz * nc) + lax.rem(mc + lax.rem(u, nc), nc))
        else:
            for zone in PLANES:

                @pl.loop(jnp.where(mz == zone, 1, 0), nx * nc)
                def _(u):
                    x = lax.rem(mx + lax.div(u, nc), nx)
                    send(q, zone * nc + x * (nz * nc) + lax.rem(mc + lax.rem(u, nc), nc))

        if q == 0:
            b_loads += [load_b(k) for k in range(1, chunks)]
            a_loads = [
                load(a, 0, a_buf.at[m], in_sem.at[m]) for m, a in enumerate((a_up, a_down))
            ]
        pack(
            q,
            [slots[me // per, me % per * CAP + r] for r in range(CAP)],
            lambda r: got[q].at[me * CAP + r],
        )

    pick_table(perm_buf, pick_vmem, me, rows, count, groups, per_group, per)
    to_smem = pltpu.make_async_copy(pick_vmem, picks, in_sem.at[3])
    to_smem.start()
    to_smem.wait()
    first = me % per * rows

    @pl.loop(0, rows)
    def _(j):
        own_picks[j] = picks[(first + j) // LANES, (first + j) % LANES]

    for a_load in a_loads:
        a_load.wait()
    for q in range(chunks):
        m, at = q // half, q % half * SUB
        every = pltpu.make_async_remote_copy(
            src_ref=sent[q].at[pl.ds(0, (count - 1) * CAP)],
            dst_ref=got[q].at[pl.ds(0, (count - 1) * CAP)],
            send_sem=send_sem.at[q],
            recv_sem=recv_sem.at[q],
            device_id={"units": me},
            device_id_type=MESH,
        )
        every.wait_recv()

        @pl.loop(0, rows // STEP)
        def _(g):
            sums = [
                a_buf[m, g * STEP + s, at : at + SUB, :] + got[q][own_picks[g * STEP + s]]
                for s in range(STEP)
            ]
            for s, value in enumerate(sums):
                merged[q][g * STEP + s] = value * 0.5

        every.wait_send()


def write_out(chunks, *refs):
    merged, outs, sem = refs[:chunks], refs[chunks:-1], refs[-1]
    half = chunks // 2
    for q in range(chunks):
        for k in range(SUB):
            column = (q % half * SUB + k) * LANES
            pltpu.make_async_copy(
                merged[q].at[:, k, :], outs[q // half].at[:, pl.ds(column, LANES)], sem.at[q]
            ).start()
    for q in range(chunks):
        pltpu.make_async_copy(merged[q], merged[q], sem.at[q]).wait()


def solution(mesh):
    nx, nz, nc = 4, 8, 2
    count = mesh.shape["units"]

    def on_device(a_up, a_down, b_up, b_down, perm):
        rows, width = a_up.shape
        chunks = 2 * width // CHUNK
        hbm = pl.BlockSpec(memory_space=pltpu.HBM)
        vmem = pl.BlockSpec(memory_space=pltpu.VMEM)
        merged = pl.pallas_call(
            functools.partial(exchange, nx, nz, nc, chunks),
            out_shape=[pltpu.VMEM((rows, SUB, LANES), jnp.float32)] * chunks,
            in_specs=[hbm] * 5,
            out_specs=[vmem] * chunks,
            scratch_shapes=[
                *[pltpu.VMEM((count * CAP, SUB, LANES), jnp.float32)] * chunks,
                *[pltpu.VMEM((count * CAP, SUB, LANES), jnp.float32)] * chunks,
                *[pltpu.VMEM((rows, SUB, LANES), jnp.float32)] * chunks,
                pltpu.VMEM((perm.shape[0] // LANES, LANES), jnp.int32),
                pltpu.VMEM((2, rows, width // LANES, LANES), jnp.float32),
                pltpu.VMEM((count // (CHUNK // rows), LANES), jnp.int32),
                pltpu.SMEM((count // (CHUNK // rows), LANES), jnp.int32),
                pltpu.VMEM((SUB, LANES), jnp.int32),
                pltpu.SMEM((SUB, LANES), jnp.int32),
                pltpu.SMEM((rows,), jnp.int32),
                pltpu.SemaphoreType.REGULAR((nz - 3,)),
                pltpu.SemaphoreType.DMA((4,)),
                pltpu.SemaphoreType.DMA((chunks,)),
                pltpu.SemaphoreType.DMA((chunks,)),
                pltpu.SemaphoreType.DMA((chunks,)),
            ],
            compiler_params=pltpu.CompilerParams(
                collective_id=0, has_side_effects=True, vmem_limit_bytes=59 * 2**20
            ),
        )(perm.reshape(-1, LANES), a_up, a_down, b_up, b_down)
        shape = jax.ShapeDtypeStruct((rows, width), jnp.float32)
        return pl.pallas_call(
            functools.partial(write_out, chunks),
            out_shape=(shape, shape),
            in_specs=[pl.BlockSpec(memory_space=pl.ANY)] * chunks,
            out_specs=(hbm, hbm),
            scratch_shapes=[pltpu.SemaphoreType.DMA((chunks,))],
            compiler_params=pltpu.CompilerParams(vmem_limit_bytes=2**20),
        )(*merged)

    units = P(("expert", "units"), None)
    return jax.shard_map(
        on_device,
        mesh=mesh,
        in_specs=(units, units, units, units, P("expert")),
        out_specs=(units, units),
        check_vma=False,
    )
```

```python
import functools

import jax
import jax.numpy as jnp
from jax import lax
from jax.experimental import pallas as pl
from jax.experimental.pallas import tpu as pltpu
from jax.sharding import PartitionSpec as P

CAP = 5
LANES = 128
SUB = 8
CHUNK = SUB * LANES
STEP = 32
Z_ORDER = (0, 4, 3, 5, 2, 6, 1, 7)
PLANES = (0, 4, 1, 5, 2, 6, 3, 7)
MESH = pl.DeviceIdType.MESH


def iota(shape, dim):
    return lax.broadcasted_iota(jnp.int32, shape, dim)


def strips(perm, groups, per_group):
    return [perm[pl.ds(r, groups, stride=per_group), :] for r in range(per_group)]


def slot_table(perm, table, me, rows, groups, per_group, per):
    lane = iota((groups, LANES), 1)
    left = []
    for strip in strips(perm, groups, per_group):
        local = strip - me * rows
        left.append(jnp.where((local >= 0) & (local < rows), local, -1))
    slots = jnp.zeros((groups, LANES), jnp.int32)
    for b in range(per):
        parts = []
        for r in range(b * rows // LANES, ((b + 1) * rows - 1) // LANES + 1):
            low, high = b * rows - r * LANES, (b + 1) * rows - r * LANES
            parts.append(jnp.where((lane >= low) & (lane < high), left[r], -1))
        for k in range(CAP):
            top = jnp.max(functools.reduce(jnp.maximum, parts), axis=1, keepdims=True)
            slots = jnp.where(lane == b * CAP + k, top, slots)
            parts = [jnp.where(part == top, -1, part) for part in parts]
    table[...] = jnp.maximum(slots, 0)


def pick_table(perm, table, me, rows, count, groups, per_group, per):
    group = me // per
    row = iota((SUB, LANES), 0)
    place = row * LANES + iota((SUB, LANES), 1)
    want = jnp.full((SUB, LANES), -1, jnp.int32)
    mine = iota((groups, LANES), 0) == group
    for r, strip in enumerate(strips(perm, groups, per_group)):
        line = jnp.max(jnp.where(mine, strip, -1), axis=0, keepdims=True)
        want = jnp.where(row == r, line, want)
    block = sum((place >= b * rows).astype(jnp.int32) for b in range(1, per))
    key = jnp.where(row < per_group, want + block * (count * rows), -1)
    whole = (key.astype(jnp.float32) + 0.5) * (1.0 / rows)
    source = whole.astype(jnp.int32)
    above = (source + 1) * rows

    def turn(s, ranks):
        for t in range(SUB):
            other = pltpu.roll(pltpu.roll(key, t, 0), s, 1)
            ranks = ranks + ((other > key) & (other < above)).astype(jnp.int32)
        return ranks

    ranks = lax.fori_loop(0, LANES, turn, jnp.zeros((SUB, LANES), jnp.int32))
    picks = (source - block * count) * CAP + ranks
    table[...] = jnp.clip(picks, 0, count * CAP - 1)


def exchange(nx, nz, nc, chunks, perm, a_up, a_down, b_up, b_down, *rest):
    merged, rest = rest[:chunks], rest[chunks:]
    sent, rest = rest[:chunks], rest[chunks:]
    got, rest = rest[:chunks], rest[chunks:]
    b_bufs, rest = rest[:chunks], rest[chunks:]
    perm_buf, a_buf, slot_vmem, slots, pick_vmem, picks, own_picks, heard, *sems = rest
    in_sem, b_sem, send_sem, recv_sem = sems
    count = nx * nz * nc
    rows, width = a_up.shape
    tiles = width // LANES
    half = tiles // SUB
    per = LANES * SUB // rows
    per_group = per * rows // LANES
    groups = count // per
    me = lax.axis_index("units")
    mx, mz, mc = lax.div(me, nz * nc), lax.rem(lax.div(me, nc), nz), lax.rem(me, nc)
    xs = [lax.rem(mx + d, nx) * (nz * nc) for d in range(nx)]
    zs = [lax.rem(mz + d, nz) * nc for d in range(nz)]
    cs = [lax.rem(mc + d, nc) for d in range(nc)]

    get_perm = pltpu.make_async_copy(perm, perm_buf, in_sem.at[2])
    get_perm.start()

    def load(src, column, dst, sem):
        for k in range(dst.shape[1]):
            pltpu.make_async_copy(
                src.at[:, pl.ds(column + k * LANES, LANES)], dst.at[:, k, :], sem
            ).start()
        return pltpu.make_async_copy(dst, dst, sem)

    def load_b(q):
        return load((b_up, b_down)[q // half], q % half * CHUNK, b_bufs[q], b_sem.at[q])

    b_loads = [load_b(0)]
    barrier = pltpu.get_barrier_semaphore()
    near = [(dz, u) for dz in (1, nz - 1, 0) for u in range(dz == 0, nx * nc)]
    for dz, u in near:
        pl.semaphore_signal(
            barrier,
            inc=1,
            device_id={"units": zs[dz] + xs[u // nc] + cs[u % nc]},
            device_id_type=MESH,
        )

    def tell(k, dz):
        pl.semaphore_signal(
            heard.at[k], inc=1, device_id={"units": zs[dz] + xs[0] + cs[0]}, device_id_type=MESH
        )

    get_perm.wait()
    slot_table(perm_buf, slot_vmem, me, rows, groups, per_group, per)
    to_smem = pltpu.make_async_copy(slot_vmem, slots, in_sem.at[3])
    to_smem.start()
    pl.semaphore_wait(barrier, len(near))
    tell(0, 1)
    tell(1, nz - 1)
    to_smem.wait()

    def pack(q, at_slots, into):
        values = [b_bufs[q][i] for i in at_slots]
        for r, value in enumerate(values):
            into(r)[...] = value

    def send(q, to):
        pltpu.make_async_remote_copy(
            src_ref=sent[q].at[pl.ds(to * CAP, CAP)],
            dst_ref=got[q].at[pl.ds(me * CAP, CAP)],
            send_sem=send_sem.at[q],
            recv_sem=recv_sem.at[q],
            device_id={"units": to},
            device_id_type=MESH,
        ).start()

    for q in range(chunks):
        b_loads[q].wait()

        @pl.loop(0, groups)
        def _(g):
            for b in range(0, per, 2):
                pack(
                    q,
                    [slots[g, b * CAP + r] for r in range(2 * CAP)],
                    lambda r: sent[q].at[(g * per + b) * CAP + r],
                )

        if q == 0:
            for dz, u in near:
                send(q, zs[dz] + xs[u // nc] + cs[u % nc])
            for step in range(2, nz // 2 + 1):
                pl.semaphore_wait(heard.at[2 * step - 4], 1)
                if step < nz // 2:
                    tell(2 * step - 2, 1)
                    pl.semaphore_wait(heard.at[2 * step - 3], 1)
                    if step + 1 < nz // 2:
                        tell(2 * step - 1, nz - 1)
                for dz in sorted({step, nz - step}):
                    for u in range(nx * nc):
                        send(q, zs[dz] + xs[u // nc] + cs[u % nc])
        elif q < chunks - 1:
            for dz in Z_ORDER:

                @pl.loop(int(dz == 0), nx * nc)
                def _(u):
                    x = lax.rem(mx + lax.div(u, nc), nx)
                    send(q, zs[dz] + x * (nz * nc) + lax.rem(mc + lax.rem(u, nc), nc))
        else:
            for zone in PLANES:

                @pl.loop(jnp.where(mz == zone, 1, 0), nx * nc)
                def _(u):
                    x = lax.rem(mx + lax.div(u, nc), nx)
                    send(q, zone * nc + x * (nz * nc) + lax.rem(mc + lax.rem(u, nc), nc))

        if q == 0:
            b_loads += [load_b(k) for k in range(1, chunks)]
            a_loads = [
                load(a, 0, a_buf.at[m], in_sem.at[m]) for m, a in enumerate((a_up, a_down))
            ]
        pack(
            q,
            [slots[me // per, me % per * CAP + r] for r in range(CAP)],
            lambda r: got[q].at[me * CAP + r],
        )

    pick_table(perm_buf, pick_vmem, me, rows, count, groups, per_group, per)
    to_smem = pltpu.make_async_copy(pick_vmem, picks, in_sem.at[3])
    to_smem.start()
    to_smem.wait()
    first = me % per * rows

    @pl.loop(0, rows)
    def _(j):
        own_picks[j] = picks[(first + j) // LANES, (first + j) % LANES]

    for a_load in a_loads:
        a_load.wait()
    for q in range(chunks):
        m, at = q // half, q % half * SUB
        every = pltpu.make_async_remote_copy(
            src_ref=sent[q].at[pl.ds(0, (count - 1) * CAP)],
            dst_ref=got[q].at[pl.ds(0, (count - 1) * CAP)],
            send_sem=send_sem.at[q],
            recv_sem=recv_sem.at[q],
            device_id={"units": me},
            device_id_type=MESH,
        )
        every.wait_recv()

        @pl.loop(0, rows // STEP)
        def _(g):
            sums = [
                a_buf[m, g * STEP + s, at : at + SUB, :] + got[q][own_picks[g * STEP + s]]
                for s in range(STEP)
            ]
            for s, value in enumerate(sums):
                merged[q][g * STEP + s] = value * 0.5

        every.wait_send()


def write_out(chunks, *refs):
    merged, outs, sem = refs[:chunks], refs[chunks:-1], refs[-1]
    half = chunks // 2
    for q in range(chunks):
        for k in range(SUB):
            column = (q % half * SUB + k) * LANES
            pltpu.make_async_copy(
                merged[q].at[:, k, :], outs[q // half].at[:, pl.ds(column, LANES)], sem.at[q]
            ).start()
    for q in range(chunks):
        pltpu.make_async_copy(merged[q], merged[q], sem.at[q]).wait()


def solution(mesh):
    nx, nz, nc = 4, 8, 2
    count = mesh.shape["units"]

    def on_device(a_up, a_down, b_up, b_down, perm):
        rows, width = a_up.shape
        chunks = 2 * width // CHUNK
        hbm = pl.BlockSpec(memory_space=pltpu.HBM)
        vmem = pl.BlockSpec(memory_space=pltpu.VMEM)
        merged = pl.pallas_call(
            functools.partial(exchange, nx, nz, nc, chunks),
            out_shape=[pltpu.VMEM((rows, SUB, LANES), jnp.float32)] * chunks,
            in_specs=[hbm] * 5,
            out_specs=[vmem] * chunks,
            scratch_shapes=[
                *[pltpu.VMEM((count * CAP, SUB, LANES), jnp.float32)] * chunks,
                *[pltpu.VMEM((count * CAP, SUB, LANES), jnp.float32)] * chunks,
                *[pltpu.VMEM((rows, SUB, LANES), jnp.float32)] * chunks,
                pltpu.VMEM((perm.shape[0] // LANES, LANES), jnp.int32),
                pltpu.VMEM((2, rows, width // LANES, LANES), jnp.float32),
                pltpu.VMEM((count // (CHUNK // rows), LANES), jnp.int32),
                pltpu.SMEM((count // (CHUNK // rows), LANES), jnp.int32),
                pltpu.VMEM((SUB, LANES), jnp.int32),
                pltpu.SMEM((SUB, LANES), jnp.int32),
                pltpu.SMEM((rows,), jnp.int32),
                pltpu.SemaphoreType.REGULAR((nz - 3,)),
                pltpu.SemaphoreType.DMA((4,)),
                pltpu.SemaphoreType.DMA((chunks,)),
                pltpu.SemaphoreType.DMA((chunks,)),
                pltpu.SemaphoreType.DMA((chunks,)),
            ],
            compiler_params=pltpu.CompilerParams(
                collective_id=0, has_side_effects=True, vmem_limit_bytes=59 * 2**20
            ),
        )(perm.reshape(-1, LANES), a_up, a_down, b_up, b_down)
        shape = jax.ShapeDtypeStruct((rows, width), jnp.float32)
        return pl.pallas_call(
            functools.partial(write_out, chunks),
            out_shape=(shape, shape),
            in_specs=[pl.BlockSpec(memory_space=pl.ANY)] * chunks,
            out_specs=(hbm, hbm),
            scratch_shapes=[pltpu.SemaphoreType.DMA((chunks,))],
            compiler_params=pltpu.CompilerParams(vmem_limit_bytes=2**20),
        )(*merged)

    units = P(("expert", "units"), None)
    return jax.shard_map(
        on_device,
        mesh=mesh,
        in_specs=(units, units, units, units, P("expert")),
        out_specs=(units, units),
        check_vma=False,
    )
```
